32 devices in a mesh: grp: 4 (over y, core), mem: 8 (over z, x).
Axes of the slice: x: 2, y: 2, z: 4, core: 2. Of those that a mesh axis runs over, the one named last changes fastest.
Arguments:
- factors: bfloat16 [64, 288, 1792], P(('grp', 'mem')), may hold values from -1.5 to 1.5
- screen: int32 [32, 18], P(('grp', 'mem')), may hold values from 0 to 1, as said below
Outputs:
- exchange_matrix: float32 [1792, 1792], P(('grp', 'mem'))
The draws below stay inside these ranges and needn't reach their ends.
Inputs may be any that keep to these rules, and one draw needn't show every extreme that they name: screen[b, j] is 1 where auxiliary block b and occupied block j survive screening; every auxiliary block keeps at least one occupied block.
All inputs are finite; a program needn't handle non-finite values.
Results may differ from the reference program's by a relative error of at most 0.0003.
Values may be sent and summed in bfloat16 or wider, within the bound.
A program may use at most 128 MiB of HBM per device.

```python
import jax
import jax.numpy as jnp
from jax import lax

NBF = 1792
NOCC = 288
NOB = 18
NAB = 32
NAUX = 64


def draw_screen(key, part):
    count_key = jax.random.fold_in(key, 11)
    shuffle_key = jax.random.fold_in(key, 23)
    kept_count = jax.random.randint(count_key, (NAB, 1), 1, NOB + 1)
    row_keys = jax.random.split(shuffle_key, NAB)

    def shuffle_row(row_key):
        return jax.random.permutation(row_key, NOB)
    shuffled = jax.vmap(shuffle_row)(row_keys)
    position = jnp.argsort(shuffled, axis=1)
    return (position < kept_count).astype(jnp.int32)


def with_spikes(array, own_key, source, target, blocks, factor):
    def block_of(dim):
        return (jnp.arange(array.shape[dim]) // (array.shape[dim] // blocks)).reshape((-1,) + (1,) * (array.ndim - 1 - dim))

    near = jax.random.permutation(own_key, blocks)[block_of(target)]
    second = (block_of(target) + blocks // 2) % blocks
    return jnp.where((block_of(source) == near) | (block_of(source) == second), factor * array, array)


def steps_of(own_key, extent, pieces, low, top_value):
    def one(axis_at, parts):
        draws = jax.random.uniform(jax.random.fold_in(jax.random.fold_in(own_key, 6), axis_at), (parts,), jnp.float32, low / len(pieces), top_value / len(pieces))
        return jnp.repeat(jnp.exp(draws), extent[axis_at] // parts).reshape((-1,) + (1,) * (len(extent) - axis_at - 1))

    level = one(*pieces[0])
    for cut in pieces[1:]:
        level = level * one(*cut)
    return level


def bell_draw_with(own_key, dims, width, most, cuts, heavy, dtype=jnp.bfloat16):
    values = width * jax.random.normal(own_key, dims, jnp.float32)
    if cuts:
        values = values * steps_of(own_key, dims, cuts, -0.22, 0.18)
    return jnp.clip(with_spikes(values, jax.random.fold_in(own_key, 3), *heavy), -most, most).astype(dtype)


def setup_inputs(seed: int = 0) -> dict:
    keys = jax.random.split(jax.random.key(seed), 3)
    factors = bell_draw_with(keys[0], (NAUX, NOCC, NBF), 0.05, 1.5, ((0, 32),), (0, 2, 32, 2.75))
    screen = draw_screen(jax.random.fold_in(keys[2], 71), 0)
    return {"factors": factors, "screen": screen}


def reference(factors, screen):
    total_aux, occ_count, basis = factors.shape
    block_count, occ_blocks = screen.shape
    aux_rows = total_aux // block_count
    occ_width = occ_count // occ_blocks
    grouped = factors.reshape(block_count, aux_rows, occ_blocks, occ_width, basis)

    def add_block(running, pair):
        block, flags = pair
        masked = block * flags.astype(jnp.bfloat16)[None, :, None, None]
        flat_rows = masked.reshape(-1, basis)
        return running + jnp.dot(flat_rows.T, flat_rows, preferred_element_type=jnp.float32), None

    result, _ = lax.scan(add_block, jnp.zeros((basis, basis), jnp.float32), (grouped, screen))
    return result
```

```python
import functools

import jax
import jax.numpy as jnp
from jax import lax
from jax.experimental import pallas as pl
from jax.experimental.pallas import tpu as pltpu
from jax.sharding import PartitionSpec as P

LANES = 128
TOP = 32767.0
MESH = pl.DeviceIdType.MESH


def bits_of(size):
    return size.bit_length() - 1


def orders_for(groups, members):
    near = [("mem", 1)]
    rows = [("grp", 2 << k) for k in range(bits_of(groups) - 1)]
    far = [("mem", 2 << k) for k in range(bits_of(members) - 1)]
    return near + rows + far, rows + near + far, far + near + rows


def kernel(
    groups, members, plan, chunks, width, x_ref, screen_ref, out_ref,
    both, turned, total, sent, got, sent_top, got_top, last,
    pair_send, pair_recv, data_send, data_recv, top_send, top_recv, end_send, end_recv,
):
    depth, basis = x_ref.shape
    own_rows = out_ref.shape[0]
    half = basis // 2
    occ_blocks = screen_ref.shape[1]
    grp, mem = lax.axis_index("grp"), lax.axis_index("mem")
    core = lax.rem(grp, 2)
    place = {"grp": grp, "mem": mem}
    levels = len(plan[0])
    starts = [0]
    for level in range(levels):
        starts.append(starts[-1] + (1 << (levels - 1 - level)))

    def peer(axis, step):
        bit = lax.rem(place[axis] // step, 2)
        there = place[axis] + (1 - 2 * bit) * step
        return (there, mem) if axis == "grp" else (grp, there)

    partner = peer("grp", 1)
    barrier = pltpu.get_barrier_semaphore()
    peers = [partner] + [peer(axis, step) for axis, step in plan[0]]
    for other in peers:
        pl.semaphore_signal(barrier, inc=1, device_id=other, device_id_type=MESH)


    def mask(j, carry):
        at = pl.ds(pl.multiple_of(j * width, width), width)
        keep = screen_ref[0, lax.rem(j, occ_blocks)].astype(jnp.float32)
        both[at, :] = (x_ref[at, :].astype(jnp.float32) * keep).astype(both.dtype)
        return carry

    pieces = 2
    piece = depth // pieces
    pair = []
    for n in range(pieces):
        lax.fori_loop(n * piece // width, (n + 1) * piece // width, mask, 0)
        if n == 0:
            pl.semaphore_wait(barrier, len(peers))
        pair.append(
            pltpu.make_async_remote_copy(
                src_ref=both.at[pl.ds(n * piece, piece)],
                dst_ref=both.at[pl.ds(depth + n * piece, piece)],
                send_sem=pair_send.at[n], recv_sem=pair_recv.at[n],
                device_id=partner, device_id_type=MESH,
            )
        )
        pair[-1].start()

    def turn(low, high):
        def one(m, carry):
            at = pl.ds(pl.multiple_of(m * 256, 256), 256)
            for k in range(low, high, LANES):
                turned[at, k : k + LANES] = both[k : k + LANES, at].T
            return carry

        lax.fori_loop(0, basis // 256, one, 0)

    early = depth // LANES * LANES
    turn(0, early)
    for copy in pair:
        copy.wait_recv()
    turn(early, 2 * depth)

    def rows_at(order, index):
        at = {"grp": grp - core, "mem": mem}
        for t, (axis, step) in enumerate(order):
            flip = index // (1 << (levels - 1 - t)) % 2
            bit = lax.rem(place[axis] // step, 2)
            at[axis] = at[axis] + flip * (1 - 2 * bit) * step
        first = (at["grp"] * members + at["mem"]) * own_rows
        second = first + members * own_rows
        return [pl.ds(pl.multiple_of(r, 8), own_rows) for r in (first, second)]

    def repeat(low, high, body):
        count = high - low
        by = 4 if count % 4 == 0 else count

        def step(t, carry):
            for u in range(by):
                body(low + t * by + u)
            return carry

        if count == by:
            step(0, 0)
        else:
            lax.fori_loop(0, count // by, step, 0)

    def columns(p):
        return slice(p * LANES, (p + 1) * LANES)

    def current(p, index, order):
        return jnp.concatenate([total[r, columns(p)] for r in rows_at(order, index)], axis=0)

    def arrived(p, level, index):
        top = got_top[p, level, pl.ds(index, 1), :]
        return got[p, starts[level] + index].astype(jnp.int32).astype(jnp.float32) * (top * (1.0 / TOP))

    def send(p, level):
        order = plan[p]
        count = 1 << (levels - 1 - level)

        def pack(i):
            value = current(p, count + i, order)
            if level:
                value = value + arrived(p, level - 1, count + i)
            top = jnp.max(jnp.abs(value), axis=0, keepdims=True)
            scale = TOP / jnp.maximum(top, 2e-34)
            sent[p, starts[level] + i] = jnp.round(value * scale).astype(jnp.int32).astype(jnp.int16)
            sent_top[p, level, pl.ds(i, 1), :] = top

        repeat(0, count, pack)
        to = peer(*order[level])
        run = pl.ds(starts[level], count)
        for here, there, a, b in (
            (sent.at[p, run], got.at[p, run], data_send, data_recv),
            (sent_top.at[p, level], got_top.at[p, level], top_send, top_recv),
        ):
            pltpu.make_async_remote_copy(
                src_ref=here, dst_ref=there, send_sem=a.at[p, level], recv_sem=b.at[p, level],
                device_id=to, device_id_type=MESH,
            ).start()

    def wait(p, level, done):
        run = pl.ds(starts[level], 1 << (levels - 1 - level))
        to = peer(*plan[p][level])
        for here, there, a, b in (
            (sent.at[p, run], got.at[p, run], data_send, data_recv),
            (sent_top.at[p, level], got_top.at[p, level], top_send, top_recv),
        ):
            copy = pltpu.make_async_remote_copy(
                src_ref=here, dst_ref=there, send_sem=a.at[p, level], recv_sem=b.at[p, level],
                device_id=to, device_id_type=MESH,
            )
            copy.wait_send() if done else copy.wait_recv()

    def keep(p, level):
        order = plan[p]

        def add(i):
            value = arrived(p, level, i)
            for n, r in enumerate(rows_at(order, i)):
                total[r, columns(p)] += value[n * own_rows : (n + 1) * own_rows]

        count = 1 << (levels - 1 - level)
        repeat(0, max(1, count // 2), add)

    parts = len(plan)
    part = 0
    for low, high in chunks:
        def multiply(m, carry):
            tall = basis // 2
            at = pl.ds(pl.multiple_of(m * tall, LANES), tall)
            total[at, low:high] = jnp.dot(
                turned[at, :],
                both[:, pl.ds(pl.multiple_of(core * half + low, LANES), high - low)],
                preferred_element_type=jnp.float32,
            )
            return carry

        lax.fori_loop(0, 2, multiply, 0)
        while part < high // LANES:
            send(part, 0)
            part += 1

    mine = pl.ds(pl.multiple_of((grp * members + mem) * own_rows, 8), own_rows)
    theirs = pl.ds(pl.multiple_of((partner[0] * members + mem) * own_rows, 8), own_rows)
    ends = []
    for level in range(levels):
        for p in range(parts):
            wait(p, level, False)
            if level + 1 < levels:
                send(p, level + 1)
            keep(p, level)
            if level + 1 == levels:
                at = pl.ds(pl.multiple_of(core * half + p * LANES, LANES), LANES)
                last[p] = total[theirs, columns(p)]
                copy = pltpu.make_async_remote_copy(
                    src_ref=last.at[p], dst_ref=out_ref.at[:, at],
                    send_sem=end_send.at[p], recv_sem=end_recv.at[p],
                    device_id=partner, device_id_type=MESH,
                )
                copy.start()
                ends.append(copy)
                out_ref[:, at] = total[mine, columns(p)]
    for copy in pair:
        copy.wait_send()
    for level in range(levels):
        for p in range(parts):
            wait(p, level, True)
    for copy in ends:
        copy.wait()


def solution(mesh):
    groups, members = mesh.shape["grp"], mesh.shape["mem"]

    def on_device(factors, screen):
        aux_rows, occ_count, basis = factors.shape
        depth = aux_rows * occ_count
        devices = groups * members
        real_rows = basis // devices
        own_rows = (real_rows + 7) // 8 * 8
        rows = factors.reshape(depth, basis)
        if own_rows != real_rows:
            rows = rows.reshape(depth, devices, real_rows)
            rows = jnp.pad(rows, ((0, 0), (0, 0), (0, own_rows - real_rows)))
            basis = devices * own_rows
            rows = rows.reshape(depth, basis)
        half = basis // 2
        parts = half // LANES
        first, second, third = orders_for(groups, members)
        plan = [(first, second, third, first, second, first, second)[p % 7] for p in range(parts)]
        chunks = [(low, min(low + 2 * LANES, half)) for low in range(0, half, 2 * LANES)]
        chips = groups * members // 2
        levels = bits_of(chips)
        block = 2 * own_rows
        places = max(8, chips // 2)
        dma = pltpu.SemaphoreType.DMA
        vmem = pl.BlockSpec(memory_space=pltpu.VMEM)
        result = pl.pallas_call(
            functools.partial(kernel, groups, members, plan, chunks, occ_count // screen.shape[1]),
            out_shape=jax.ShapeDtypeStruct((own_rows, basis), jnp.float32),
            in_specs=[vmem, pl.BlockSpec(memory_space=pltpu.SMEM)],
            out_specs=vmem,
            scratch_shapes=[
                pltpu.VMEM((2 * depth, basis), jnp.bfloat16),
                pltpu.VMEM((basis, 2 * depth), jnp.bfloat16),
                pltpu.VMEM((basis, half), jnp.float32),
                pltpu.VMEM((parts, chips - 1, block, LANES), jnp.int16),
                pltpu.VMEM((parts, chips - 1, block, LANES), jnp.int16),
                pltpu.VMEM((parts, levels, places, LANES), jnp.float32),
                pltpu.VMEM((parts, levels, places, LANES), jnp.float32),
                pltpu.VMEM((parts, own_rows, LANES), jnp.float32),
                dma((2,)), dma((2,)),
                dma((parts, levels)), dma((parts, levels)),
                dma((parts, levels)), dma((parts, levels)),
                dma((parts,)), dma((parts,)),
            ],
            compiler_params=pltpu.CompilerParams(
                collective_id=0, has_side_effects=True, vmem_limit_bytes=60 * 1024 * 1024
            ),
        )(rows, screen)
        if own_rows != real_rows:
            result = result[:real_rows].reshape(real_rows, devices, own_rows)[:, :, :real_rows]
            result = result.reshape(real_rows, devices * real_rows)
        return result

    placed = (P(("grp", "mem"), None, None), P(("grp", "mem"), None))
    return jax.shard_map(
        on_device, mesh=mesh, in_specs=placed, out_specs=P(("grp", "mem"), None), check_vma=False
    )
```

```python
import functools

import jax
import jax.numpy as jnp
from jax import lax
from jax.experimental import pallas as pl
from jax.experimental.pallas import tpu as pltpu
from jax.sharding import PartitionSpec as P

LANES = 128
TOP = 32767.0
KINDS = "DGCFGFG"
STEPS = [0, 1, 2, 3, 4, 0, 1, 5, 6, 2, 3, 4, 0, 1, 5, 6]
MESH = pl.DeviceIdType.MESH


def bits_of(size):
    return size.bit_length() - 1


def plan_for(groups, members, parts):
    near = [[("mem", 1)]]
    rows = [[("grp", 2 << k)] for k in range(bits_of(groups) - 1)]
    far = [("mem", 2 << k) for k in range(bits_of(members) - 1)]
    single = [[bit] for bit in far]
    direct = [far[k : k + 2][::-1] for k in range(0, len(far), 2)]
    kinds = {
        "A": near + rows + direct,
        "B": rows + near + direct,
        "C": single + near + rows,
        "D": near + single + rows,
        "E": rows + single + near,
        "F": near + rows + single,
        "G": rows + near + single,
    }
    return [kinds[KINDS[p % len(KINDS)]] for p in range(parts)]


def messages_of(stages):
    left = 1
    for bits in stages:
        left <<= len(bits)
    result, slot = [], 0
    for level, bits in enumerate(stages):
        left >>= len(bits)
        for target in range(1, 1 << len(bits)):
            result.append((level, target, target * left, left, slot))
            slot += left
    return result


def kernel(
    groups, members, plan, chunks, width, x_ref, screen_ref, out_ref,
    both, turned, total, sent, got, sent_top, got_top, last,
    pair_send, pair_recv, data_send, data_recv, top_send, top_recv, end_send, end_recv,
):
    depth, basis = x_ref.shape
    own_rows = out_ref.shape[0]
    half = basis // 2
    occ_blocks = screen_ref.shape[1]
    grp, mem = lax.axis_index("grp"), lax.axis_index("mem")
    core = lax.rem(grp, 2)
    place = {"grp": grp, "mem": mem}
    def peer(bits):
        there = dict(place)
        for axis, step in bits:
            bit = lax.rem(place[axis] // step, 2)
            there[axis] = there[axis] + (1 - 2 * bit) * step
        return there["grp"], there["mem"]

    def chosen(bits, target):
        return tuple(b for t, b in enumerate(bits) if target >> (len(bits) - 1 - t) & 1)

    partner = peer([("grp", 1)])
    barrier = pltpu.get_barrier_semaphore()
    met = {
        tuple(sorted(chosen(stages[level], target)))
        for stages in plan
        for level, target, *_ in messages_of(stages)
    }
    peers = [partner] + [peer(bits) for bits in sorted(met)]
    for other in peers:
        pl.semaphore_signal(barrier, inc=1, device_id=other, device_id_type=MESH)


    def mask(j, carry):
        at = pl.ds(pl.multiple_of(j * width, width), width)
        keep = screen_ref[0, lax.rem(j, occ_blocks)].astype(jnp.float32)
        both[at, :] = (x_ref[at, :].astype(jnp.float32) * keep).astype(both.dtype)
        return carry

    pieces = 2
    piece = depth // pieces
    pair = []
    for n in range(pieces):
        lax.fori_loop(n * piece // width, (n + 1) * piece // width, mask, 0)
        if n == 0:
            pl.semaphore_wait(barrier, len(peers))
        pair.append(
            pltpu.make_async_remote_copy(
                src_ref=both.at[pl.ds(n * piece, piece)],
                dst_ref=both.at[pl.ds(depth + n * piece, piece)],
                send_sem=pair_send.at[n], recv_sem=pair_recv.at[n],
                device_id=partner, device_id_type=MESH,
            )
        )
        pair[-1].start()

    def turn(low, high):
        def one(m, carry):
            at = pl.ds(pl.multiple_of(m * 256, 256), 256)
            for k in range(low, high, LANES):
                turned[at, k : k + LANES] = both[k : k + LANES, at].T
            return carry

        lax.fori_loop(0, basis // 256, one, 0)

    early = depth // LANES * LANES
    turn(0, early)
    for copy in pair:
        copy.wait_recv()
    turn(early, 2 * depth)

    def rows_at(stages, index):
        order = [bit for bits in stages for bit in bits]
        at = {"grp": grp - core, "mem": mem}
        for t, (axis, step) in enumerate(order):
            flip = index // (1 << (len(order) - 1 - t)) % 2
            bit = lax.rem(place[axis] // step, 2)
            at[axis] = at[axis] + flip * (1 - 2 * bit) * step
        first = (at["grp"] * members + at["mem"]) * own_rows
        second = first + members * own_rows
        return [pl.ds(pl.multiple_of(r, 8), own_rows) for r in (first, second)]

    def repeat(low, high, body):
        count = high - low
        by = 4 if count % 4 == 0 else count

        def step(t, carry):
            for u in range(by):
                body(low + t * by + u)
            return carry

        if count == by:
            step(0, 0)
        else:
            lax.fori_loop(0, count // by, step, 0)

    def columns(p):
        return slice(p * LANES, (p + 1) * LANES)

    def current(p, index, order):
        return jnp.concatenate([total[r, columns(p)] for r in rows_at(order, index)], axis=0)

    def arrived(p, level, index):
        value = None
        for m, (at, _, _, _, slot) in enumerate(messages_of(plan[p])):
            if at == level:
                top = got_top[p, m, pl.ds(index, 1), :] * (1.0 / TOP)
                one = got[p, slot + index].astype(jnp.int32).astype(jnp.float32) * top
                value = one if value is None else value + one
        return value

    def copies(p, m):
        level, target, _, count, slot = messages_of(plan[p])[m]
        run = pl.ds(slot, count)
        to = peer(chosen(plan[p][level], target))
        return [
            pltpu.make_async_remote_copy(
                src_ref=here, dst_ref=there, send_sem=a.at[p, m], recv_sem=b.at[p, m],
                device_id=to, device_id_type=MESH,
            )
            for here, there, a, b in (
                (sent.at[p, run], got.at[p, run], data_send, data_recv),
                (sent_top.at[p, m], got_top.at[p, m], top_send, top_recv),
            )
        ]

    def send(p, level):
        for m, (at, _, first, count, slot) in reversed(list(enumerate(messages_of(plan[p])))):
            if at != level:
                continue

            def pack(i):
                value = current(p, first + i, plan[p])
                if level:
                    value = value + arrived(p, level - 1, first + i)
                top = jnp.max(jnp.abs(value), axis=0, keepdims=True)
                scale = TOP / jnp.maximum(top, 2e-34)
                sent[p, slot + i] = jnp.round(value * scale).astype(jnp.int32).astype(jnp.int16)
                sent_top[p, m, pl.ds(i, 1), :] = top

            repeat(0, count, pack)
            for copy in copies(p, m):
                copy.start()

    def wait(p, level):
        for m, (at, *_) in enumerate(messages_of(plan[p])):
            if at == level:
                for copy in copies(p, m):
                    copy.wait_recv()

    def keep(p, level):
        count = [n for at, _, _, n, _ in messages_of(plan[p]) if at == level][0]
        if level + 1 < len(plan[p]):
            count >>= len(plan[p][level + 1])

        def add(i):
            value = arrived(p, level, i)
            for n, r in enumerate(rows_at(plan[p], i)):
                total[r, columns(p)] += value[n * own_rows : (n + 1) * own_rows]

        repeat(0, count, add)

    parts = len(plan)
    mine = pl.ds(pl.multiple_of((grp * members + mem) * own_rows, 8), own_rows)
    theirs = pl.ds(pl.multiple_of((partner[0] * members + mem) * own_rows, 8), own_rows)
    ends = []

    def advance(p, level):
        wait(p, level)
        if level + 1 < len(plan[p]):
            send(p, level + 1)
            keep(p, level)
            return
        keep(p, level)
        last[p] = total[theirs, columns(p)]
        at = pl.ds(pl.multiple_of(core * half + p * LANES, LANES), LANES)
        copy = pltpu.make_async_remote_copy(
            src_ref=last.at[p], dst_ref=out_ref.at[:, at],
            send_sem=end_send.at[p], recv_sem=end_recv.at[p],
            device_id=partner, device_id_type=MESH,
        )
        copy.start()
        ends.append(copy)
        out_ref[:, at] = total[mine, columns(p)]

    def multiply(low, high):
        def one(m, carry):
            tall = basis // 2
            at = pl.ds(pl.multiple_of(m * tall, LANES), tall)
            total[at, low:high] = jnp.dot(
                turned[at, :],
                both[:, pl.ds(pl.multiple_of(core * half + low, LANES), high - low)],
                preferred_element_type=jnp.float32,
            )
            return carry

        lax.fori_loop(0, 2, one, 0)

    step = [0] * parts
    made = 0
    for p in STEPS + list(range(parts)) * (2 + max(len(stages) for stages in plan)):
        if p >= parts or step[p] > len(plan[p]):
            continue
        if step[p] == 0:
            while chunks[made][0] <= p * LANES if made < len(chunks) else False:
                multiply(*chunks[made])
                made += 1
            send(p, 0)
        else:
            advance(p, step[p] - 1)
        step[p] += 1
    for copy in pair:
        copy.wait_send()
    for p in range(parts):
        for m in range(len(messages_of(plan[p]))):
            for copy in copies(p, m):
                copy.wait_send()
    for copy in ends:
        copy.wait()


def solution(mesh):
    groups, members = mesh.shape["grp"], mesh.shape["mem"]

    def on_device(factors, screen):
        aux_rows, occ_count, basis = factors.shape
        depth = aux_rows * occ_count
        devices = groups * members
        real_rows = basis // devices
        own_rows = (real_rows + 7) // 8 * 8
        rows = factors.reshape(depth, basis)
        if own_rows != real_rows:
            rows = rows.reshape(depth, devices, real_rows)
            rows = jnp.pad(rows, ((0, 0), (0, 0), (0, own_rows - real_rows)))
            basis = devices * own_rows
            rows = rows.reshape(depth, basis)
        half = basis // 2
        parts = half // LANES
        plan = plan_for(groups, members, parts)
        chunks = [(low, min(low + 2 * LANES, half)) for low in range(0, half, 2 * LANES)]
        chips = groups * members // 2
        levels = max(len(messages_of(stages)) for stages in plan)
        block = 2 * own_rows
        places = max(8, chips // 2)
        dma = pltpu.SemaphoreType.DMA
        vmem = pl.BlockSpec(memory_space=pltpu.VMEM)
        result = pl.pallas_call(
            functools.partial(kernel, groups, members, plan, chunks, occ_count // screen.shape[1]),
            out_shape=pltpu.VMEM((own_rows, basis), jnp.float32),
            in_specs=[vmem, pl.BlockSpec(memory_space=pltpu.SMEM)],
            out_specs=vmem,
            scratch_shapes=[
                pltpu.VMEM((2 * depth, basis), jnp.bfloat16),
                pltpu.VMEM((basis, 2 * depth), jnp.bfloat16),
                pltpu.VMEM((basis, half), jnp.float32),
                pltpu.VMEM((parts, chips - 1, block, LANES), jnp.int16),
                pltpu.VMEM((parts, chips - 1, block, LANES), jnp.int16),
                pltpu.VMEM((parts, levels, places, LANES), jnp.float32),
                pltpu.VMEM((parts, levels, places, LANES), jnp.float32),
                pltpu.VMEM((parts, own_rows, LANES), jnp.float32),
                dma((2,)), dma((2,)),
                dma((parts, levels)), dma((parts, levels)),
                dma((parts, levels)), dma((parts, levels)),
                dma((parts,)), dma((parts,)),
            ],
            compiler_params=pltpu.CompilerParams(
                collective_id=0, has_side_effects=True, vmem_limit_bytes=60 * 1024 * 1024
            ),
        )(rows, screen)
        if own_rows != real_rows:
            result = result[:real_rows].reshape(real_rows, devices, own_rows)[:, :, :real_rows]
            result = result.reshape(real_rows, devices * real_rows)
        return result

    placed = (P(("grp", "mem"), None, None), P(("grp", "mem"), None))
    return jax.shard_map(
        on_device, mesh=mesh, in_specs=placed, out_specs=P(("grp", "mem"), None), check_vma=False
    )
```
